32 devices in a mesh: south: 4 (over y, x), east: 4 (over z), down: 2 (over core).
Axes of the slice: x: 2, y: 2, z: 4, core: 2. Of those that a mesh axis runs over, the one named last changes fastest.
Arguments:
- field_values: float32 [32, 384, 16, 128], P('south', 'east', 'down'), may hold values from 0.2 to 1.8
- flow_y: float32 [32, 384, 16, 128], P('south', 'east', 'down'), may hold values from -0.3 to 0.3
- flow_x: float32 [32, 384, 16, 128], P('south', 'east', 'down'), may hold values from -0.3 to 0.3
- flow_z: float32 [32, 384, 16, 128], P('south', 'east', 'down'), may hold values from -0.3 to 0.3
Outputs:
- potential: float32 [32, 384, 16, 128], P('south', 'east', 'down')
- field_values_end: float32 [32, 384, 16, 128], P('south', 'east', 'down')
The draws below stay inside these ranges and needn't reach their ends.
All inputs are finite; a program needn't handle non-finite values.
Results may differ from the reference program's by a relative error of at most 0.00002.
Values sent between devices are 32-bit elements; how exact they have to be, the bound alone decides.
A program may use at most 128 MiB of HBM per device.

```python
import jax
import jax.numpy as jnp
from jax import lax

GRID_Y = 32
GRID_X = 384
GRID_Z = 16
LEVELS = 128
STEPS = 4


def level_of(own_key, extent, cuts, low, largest):
    factor_of = 1.0
    for position, parts in cuts:
        steps = jax.random.uniform(jax.random.fold_in(jax.random.fold_in(own_key, 6), position), (parts,), jnp.float32, low / len(cuts), largest / len(cuts))
        factor_of = factor_of * jnp.repeat(jnp.exp(steps), extent[position] // parts).reshape((-1,) + (1,) * (len(extent) - 1 - position))
    return factor_of


def setup_inputs(seed: int = 0) -> dict:
    seeds = jax.random.split(jax.random.key(seed), 5)
    field_values = jnp.clip(0.2 + 1.5999999 * jax.random.uniform(seeds[0], (GRID_Y, GRID_X, GRID_Z, LEVELS), jnp.float32) ** level_of(seeds[0], (GRID_Y, GRID_X, GRID_Z, LEVELS), ((0, 4), (1, 4), (2, 2)), -0.2, 0.2), 0.2, 1.8)
    flow_y = jnp.clip(jax.random.uniform(seeds[1], (GRID_Y, GRID_X, GRID_Z, LEVELS), jnp.float32, -0.3, 0.3) * level_of(seeds[1], (GRID_Y, GRID_X, GRID_Z, LEVELS), ((0, 4), (1, 4), (2, 2)), -0.4, 0.0), -0.3, 0.3)
    flow_x = jnp.clip(jax.random.uniform(seeds[2], (GRID_Y, GRID_X, GRID_Z, LEVELS), jnp.float32, -0.3, 0.3) * level_of(seeds[2], (GRID_Y, GRID_X, GRID_Z, LEVELS), ((0, 4), (1, 4), (2, 2)), -0.4, 0.0), -0.3, 0.3)
    flow_z = jnp.clip(jax.random.uniform(seeds[3], (GRID_Y, GRID_X, GRID_Z, LEVELS), jnp.float32, -0.3, 0.3) * level_of(seeds[3], (GRID_Y, GRID_X, GRID_Z, LEVELS), ((0, 4), (1, 4), (2, 2)), -0.4, 0.0), -0.3, 0.3)
    return {"field_values": field_values, "flow_y": flow_y, "flow_x": flow_x, "flow_z": flow_z}


def without_rim(values, dims):
    for dim in dims:
        values = lax.slice_in_dim(values, 1, values.shape[dim] - 1, axis=dim)
    return values


def shifted_cells(values, dim, start, dims):
    others = [other for other in dims if other != dim]
    values = without_rim(values, others)
    return lax.slice_in_dim(values, start, start + values.shape[dim] - 2, axis=dim)


def march_step(padded, flow_y, flow_x, flow_z):
    middle = without_rim(padded, (0, 1, 2))
    lower = [shifted_cells(padded, dim, 0, (0, 1, 2)) for dim in (0, 1, 2)]
    upper = [shifted_cells(padded, dim, 2, (0, 1, 2)) for dim in (0, 1, 2)]
    slopes = [above - below for above, below in zip(upper, lower)]
    smooth_rate = 0.05
    spread = lower[0] + upper[0] + lower[1] + upper[1] + lower[2] + upper[2] - 6.0 * middle
    return middle - flow_y * slopes[0] - flow_x * slopes[1] - flow_z * slopes[2] + smooth_rate * spread


def reference(field_values, flow_y, flow_x, flow_z):
    for step in range(STEPS):
        field_values = march_step(jnp.pad(field_values, ((1, 1), (1, 1), (1, 1), (0, 0)), mode="wrap"), flow_y, flow_x, flow_z)
    potential = jnp.cumsum(field_values, axis=2) / GRID_Z
    return potential, field_values
```

```python
import functools

import jax
import jax.numpy as jnp
from jax import lax
from jax.experimental import pallas as pl
from jax.experimental.pallas import tpu as pltpu
from jax.sharding import PartitionSpec as P

STEPS = 4
AXES = ("south", "east", "down")
MESH = pl.DeviceIdType.MESH


def group_of(columns):
    return next(size for size in (8, 4, 2, 1) if columns % size == 0)


def chunk_of(columns, group):
    return next(size for size in (2 * group, group) if columns % size == 0)


def kernel(sizes, depth, field, flow_y, flow_x, flow_z, pot_out, end_out, u, end, pot, fy, fx, fz,
           faces, halos, totals, totals_in, load_sem, store_sem, south_send, south_recv,
           east_send, east_recv, down_send, down_recv, tot_send, tot_recv):
    rows, cells, levels = field.shape
    columns = cells // depth
    group = group_of(columns)
    width = chunk_of(columns, group)
    chunks = columns // width
    places = {axis: lax.axis_index(axis) for axis in AXES}

    def beside(axis, hop):
        return {axis: lax.rem(places[axis] + hop, sizes[axis])}

    hops = [(axis, hop) for axis in ("south", "east") for hop in sorted({1, sizes[axis] - 1})]
    hops += [("down", hop) for hop in range(1, sizes["down"])]
    barrier = pltpu.get_barrier_semaphore()
    for axis, hop in hops:
        pl.semaphore_signal(barrier, inc=1, device_id=beside(axis, hop), device_id_type=MESH)

    flows = ((flow_y, fy), (flow_x, fx), (flow_z, fz))
    loads = [pltpu.make_async_copy(field, u.at[0, pl.ds(1, rows), pl.ds(depth, cells), :], load_sem.at[0])]
    loads += [pltpu.make_async_copy(src, dst, load_sem.at[1 + i]) for i, (src, dst) in enumerate(flows)]
    for load in loads:
        load.start()
    pl.semaphore_wait(barrier, len(hops))

    def south(t, side, c):
        row = rows - 1 if side == 0 else 0
        at = pl.multiple_of(c * width * depth, 8)
        if t == 0:
            src = field.at[row, pl.ds(at, width * depth), :]
        else:
            src = u.at[t, row + 1, pl.ds(at + depth, width * depth), :]
        return pltpu.make_async_remote_copy(
            src_ref=src,
            dst_ref=u.at[t, 0 if side == 0 else rows + 1, pl.ds(at + depth, width * depth), :],
            send_sem=south_send.at[t, side, c], recv_sem=south_recv.at[t, side, c],
            device_id=beside("south", 1 if side == 0 else sizes["south"] - 1), device_id_type=MESH)

    blocks = ((1, rows - 2), (0, 1), (rows - 1, 1))

    def east(t, side, part):
        start, count = blocks[part]
        column = columns if side == 0 else 1
        if t == 0:
            src = field.at[pl.ds(start, count), pl.ds((column - 1) * depth, depth), :]
        else:
            src = u.at[t, pl.ds(start + 1, count), pl.ds(column * depth, depth), :]
        return pltpu.make_async_remote_copy(
            src_ref=src,
            dst_ref=u.at[t, pl.ds(start + 1, count), pl.ds(0 if side == 0 else cells + depth, depth), :],
            send_sem=east_send.at[t, side, part], recv_sem=east_recv.at[t, side, part],
            device_id=beside("east", 1 if side == 0 else sizes["east"] - 1), device_id_type=MESH)

    def down(t, side, part):
        start, count = blocks[part]
        return pltpu.make_async_remote_copy(
            src_ref=faces.at[t, side, pl.ds(start, count)],
            dst_ref=halos.at[t, side, pl.ds(start, count)],
            send_sem=down_send.at[t, side, part], recv_sem=down_recv.at[t, side, part],
            device_id=beside("down", 1 if side == 0 else sizes["down"] - 1), device_id_type=MESH)

    def total(hop, part):
        start, count = blocks[part]
        return pltpu.make_async_remote_copy(
            src_ref=totals.at[pl.ds(start, count)],
            dst_ref=totals_in.at[hop - 1, pl.ds(start, count)],
            send_sem=tot_send.at[hop - 1, part], recv_sem=tot_recv.at[hop - 1, part],
            device_id=beside("down", hop), device_id_type=MESH)

    place_in_block = lax.broadcasted_iota(jnp.int32, (depth, levels), 0)
    on_first, on_last = place_in_block == 0, place_in_block == depth - 1

    def take_faces(t, y, x0):
        for side, place in ((0, depth - 1), (1, 0)):
            start = (x0 + 1) * depth + place
            faces[t, side, y, pl.ds(x0, group), :] = u[t, y + 1, pl.ds(start, group, stride=depth), :]

    def march(t, y, x0):
        def at(x, pad):
            return pl.ds(pl.multiple_of((x + pad) * depth, 8), depth)

        line = [u[t - 1, y + 1, at(x0 + g, 0), :] for g in range(group + 2)]
        for g in range(group):
            x = x0 + g
            mid, west, east_of = line[g + 1], line[g], line[g + 2]
            north, south_of = u[t - 1, y, at(x, 1), :], u[t - 1, y + 2, at(x, 1), :]
            low = jnp.broadcast_to(halos[t - 1, 0, y, pl.ds(x, 1), :], (depth, levels))
            high = jnp.broadcast_to(halos[t - 1, 1, y, pl.ds(x, 1), :], (depth, levels))
            low = jnp.where(on_first, low, pltpu.roll(mid, 1, 0))
            high = jnp.where(on_last, high, pltpu.roll(mid, depth - 1, 0))
            own = at(x, 0)
            spread = (north + south_of) + (west + east_of) + (low + high) - 6.0 * mid
            value = (mid - fy[y, own, :] * (south_of - north) - fx[y, own, :] * (east_of - west)
                     - fz[y, own, :] * (high - low) + 0.05 * spread)
            if t < STEPS:
                u[t, y + 1, at(x, 1), :] = value
            else:
                end[y, own, :] = value
                hop = 1
                while hop < depth:
                    value = value + jnp.where(place_in_block >= hop, pltpu.roll(value, hop, 0), 0.0)
                    hop *= 2
                pot[y, own, :] = value
        if t < STEPS:
            take_faces(t, y, x0)
        else:
            start = x0 * depth + depth - 1
            totals[y, pl.ds(x0, group), :] = pot[y, pl.ds(start, group, stride=depth), :]

    def over(y0, count, x0, span, body):
        groups = span // group

        def one(i, carry):
            body(y0 + i // groups, pl.multiple_of(x0 + (i % groups) * group, group))
            return carry

        lax.fori_loop(0, count * groups, one, 0)

    def finish(part):
        for hop in range(1, sizes["down"]):
            total(hop, part).wait_recv()

        def one(y, x0):
            for g in range(group):
                own = pl.ds(pl.multiple_of((x0 + g) * depth, 8), depth)
                value = pot[y, own, :]
                for hop in range(1, sizes["down"]):
                    below = jnp.broadcast_to(totals_in[hop - 1, y, pl.ds(x0 + g, 1), :], (depth, levels))
                    value = value + jnp.where(places["down"] >= hop, below, 0.0)
                pot[y, own, :] = value / (depth * sizes["down"])

        over(*blocks[part], 0, columns, one)

    def stores(part):
        start, count = blocks[part]
        cut = pl.ds(start, count)
        return (pltpu.make_async_copy(end.at[cut], end_out.at[cut], store_sem.at[0, part]),
                pltpu.make_async_copy(pot.at[cut], pot_out.at[cut], store_sem.at[1, part]))

    def each_chunk(body):
        def one(c, carry):
            body(c)
            return carry

        lax.fori_loop(0, chunks, one, 0)

    def send_chunk(t, c):
        for side in (0, 1):
            south(t, side, c).start()

    each_chunk(lambda c: send_chunk(0, c))
    for part in (0, 1, 2):
        for side in (0, 1):
            east(0, side, part).start()
    loads[0].wait()
    for part in (0, 1, 2):
        over(*blocks[part], 0, columns, functools.partial(take_faces, 0))
        for side in (0, 1):
            down(0, side, part).start()
    for load in loads[1:]:
        load.wait()

    for t in range(1, STEPS + 1):
        for side in (0, 1):
            east(t - 1, side, 0).wait_recv()
            down(t - 1, side, 0).wait_recv()
        over(*blocks[0], 0, columns, functools.partial(march, t))
        if t < STEPS:
            for side in (0, 1):
                east(t, side, 0).start()
                down(t, side, 0).start()
        else:
            stores(0)[0].start()
            for hop in range(1, sizes["down"]):
                total(hop, 0).start()
            finish(0)
            stores(0)[1].start()
        for part in (1, 2):
            for side in (0, 1):
                east(t - 1, side, part).wait_recv()
                down(t - 1, side, part).wait_recv()

        def rim(c):
            for side in (0, 1):
                south(t - 1, side, c).wait_recv()
                y = 0 if side == 0 else rows - 1
                over(y, 1, c * width, width, functools.partial(march, t))
            if t < STEPS:
                send_chunk(t, c)

        each_chunk(rim)
        for part in (1, 2):
            if t < STEPS:
                for side in (0, 1):
                    east(t, side, part).start()
                    down(t, side, part).start()
            else:
                stores(part)[0].start()
                for hop in range(1, sizes["down"]):
                    total(hop, part).start()
    for part in (1, 2):
        finish(part)
        stores(part)[1].start()
    for t in range(STEPS):
        each_chunk(lambda c: [south(t, side, c).wait_send() for side in (0, 1)])
        for part in (0, 1, 2):
            for side in (0, 1):
                east(t, side, part).wait_send()
                down(t, side, part).wait_send()
    for part in (0, 1, 2):
        for hop in range(1, sizes["down"]):
            total(hop, part).wait_send()
        for store in stores(part):
            store.wait()


def local(sizes, field_values, *flows):
    rows, columns, depth, levels = field_values.shape
    cells = columns * depth
    width = chunk_of(columns, group_of(columns))
    flat = [array.reshape(rows, cells, levels) for array in (field_values, *flows)]
    block = pltpu.VMEM((rows, cells, levels), jnp.float32)
    dma = pltpu.SemaphoreType.DMA
    south_sems, side_sems = (STEPS, 2, columns // width), (STEPS, 2, 3)
    others = sizes["down"] - 1
    face = (rows, columns, levels)
    out = jax.ShapeDtypeStruct((rows, cells, levels), jnp.float32)
    results = pl.pallas_call(
        functools.partial(kernel, sizes, depth),
        out_shape=(out, out),
        in_specs=[pl.BlockSpec(memory_space=pl.ANY)] * 4,
        out_specs=(pl.BlockSpec(memory_space=pl.ANY),) * 2,
        scratch_shapes=[
            pltpu.VMEM((STEPS, rows + 2, cells + 2 * depth, levels), jnp.float32),
            block, block, block, block, block,
            pltpu.VMEM((STEPS, 2, *face), jnp.float32),
            pltpu.VMEM((STEPS, 2, *face), jnp.float32),
            pltpu.VMEM(face, jnp.float32),
            pltpu.VMEM((others, *face), jnp.float32),
            dma((4,)), dma((2, 3)),
            dma(south_sems), dma(south_sems),
            dma(side_sems), dma(side_sems),
            dma(side_sems), dma(side_sems),
            dma((others, 3)), dma((others, 3)),
        ],
        compiler_params=pltpu.CompilerParams(
            collective_id=0, has_side_effects=True, vmem_limit_bytes=60 * 1024 * 1024),
    )(*flat)
    return tuple(array.reshape(rows, columns, depth, levels) for array in results)


def solution(mesh):
    spec = P("south", "east", "down", None)
    sizes = {axis: mesh.shape[axis] for axis in AXES}
    return jax.shard_map(
        functools.partial(local, sizes), mesh=mesh, in_specs=(spec,) * 4,
        out_specs=(spec, spec), check_vma=False)
```

```python
import functools

import jax
import jax.numpy as jnp
from jax import lax
from jax.experimental import pallas as pl
from jax.experimental.pallas import tpu as pltpu
from jax.sharding import PartitionSpec as P

STEPS = 4
AXES = ("south", "east", "down")
MESH = pl.DeviceIdType.MESH


def group_of(columns):
    return next(size for size in (8, 4, 2, 1) if columns % size == 0)


def chunk_of(columns, group):
    return next(size for size in (2 * group, group) if columns % size == 0)


def kernel(sizes, depth, field, flow_y, flow_x, flow_z, pot, end, u, fy, fx, fz,
           faces, halos, totals, totals_in, load_sem, south_send, south_recv,
           east_send, east_recv, down_send, down_recv, tot_send, tot_recv):
    rows, cells, levels = field.shape
    columns = cells // depth
    group = group_of(columns)
    width = chunk_of(columns, group)
    chunks = columns // width
    places = {axis: lax.axis_index(axis) for axis in AXES}

    def beside(axis, hop):
        return {axis: lax.rem(places[axis] + hop, sizes[axis])}

    hops = [(axis, hop) for axis in ("south", "east") for hop in sorted({1, sizes[axis] - 1})]
    hops += [("down", hop) for hop in range(1, sizes["down"])]
    barrier = pltpu.get_barrier_semaphore()
    for axis, hop in hops:
        pl.semaphore_signal(barrier, inc=1, device_id=beside(axis, hop), device_id_type=MESH)

    flows = ((flow_y, fy), (flow_x, fx), (flow_z, fz))
    loads = [pltpu.make_async_copy(field, u.at[0, pl.ds(1, rows), pl.ds(depth, cells), :], load_sem.at[0])]
    loads += [pltpu.make_async_copy(src, dst, load_sem.at[1 + i]) for i, (src, dst) in enumerate(flows)]
    for load in loads:
        load.start()
    pl.semaphore_wait(barrier, len(hops))

    def south(t, side, c):
        row = rows - 1 if side == 0 else 0
        at = pl.multiple_of(c * width * depth, 8)
        if t == 0:
            src = field.at[row, pl.ds(at, width * depth), :]
        else:
            src = u.at[t, row + 1, pl.ds(at + depth, width * depth), :]
        return pltpu.make_async_remote_copy(
            src_ref=src,
            dst_ref=u.at[t, 0 if side == 0 else rows + 1, pl.ds(at + depth, width * depth), :],
            send_sem=south_send.at[t, side, c], recv_sem=south_recv.at[t, side, c],
            device_id=beside("south", 1 if side == 0 else sizes["south"] - 1), device_id_type=MESH)

    blocks = ((1, rows - 2), (0, 1), (rows - 1, 1))

    def east(t, side, part):
        start, count = blocks[part]
        column = columns if side == 0 else 1
        if t == 0:
            src = field.at[pl.ds(start, count), pl.ds((column - 1) * depth, depth), :]
        else:
            src = u.at[t, pl.ds(start + 1, count), pl.ds(column * depth, depth), :]
        return pltpu.make_async_remote_copy(
            src_ref=src,
            dst_ref=u.at[t, pl.ds(start + 1, count), pl.ds(0 if side == 0 else cells + depth, depth), :],
            send_sem=east_send.at[t, side, part], recv_sem=east_recv.at[t, side, part],
            device_id=beside("east", 1 if side == 0 else sizes["east"] - 1), device_id_type=MESH)

    def down(t, side, part):
        start, count = blocks[part]
        return pltpu.make_async_remote_copy(
            src_ref=faces.at[t, side, pl.ds(start, count)],
            dst_ref=halos.at[t, side, pl.ds(start, count)],
            send_sem=down_send.at[t, side, part], recv_sem=down_recv.at[t, side, part],
            device_id=beside("down", 1 if side == 0 else sizes["down"] - 1), device_id_type=MESH)

    def total(hop, piece, y0, count, x0, span):
        cut = (pl.ds(y0, count), pl.ds(x0, span))
        return pltpu.make_async_remote_copy(
            src_ref=totals.at[cut], dst_ref=totals_in.at[(hop - 1, *cut)],
            send_sem=tot_send.at[hop - 1, piece], recv_sem=tot_recv.at[hop - 1, piece],
            device_id=beside("down", hop), device_id_type=MESH)

    def inner_total(hop):
        return total(hop, 0, *blocks[0], 0, columns)

    def rim_total(hop, side, c):
        at = pl.multiple_of(c * width, group)
        return total(hop, 1 + side * chunks + c, 0 if side == 0 else rows - 1, 1, at, width)

    place_in_block = lax.broadcasted_iota(jnp.int32, (depth, levels), 0)
    on_first, on_last = place_in_block == 0, place_in_block == depth - 1

    def take_faces(t, y, x0):
        for side, place in ((0, depth - 1), (1, 0)):
            start = (x0 + 1) * depth + place
            faces[t, side, y, pl.ds(x0, group), :] = u[t, y + 1, pl.ds(start, group, stride=depth), :]

    def march(t, y, x0):
        def at(x, pad):
            return pl.ds(pl.multiple_of((x + pad) * depth, 8), depth)

        line = [u[t - 1, y + 1, at(x0 + g, 0), :] for g in range(group + 2)]
        for g in range(group):
            x = x0 + g
            mid, west, east_of = line[g + 1], line[g], line[g + 2]
            north, south_of = u[t - 1, y, at(x, 1), :], u[t - 1, y + 2, at(x, 1), :]
            low = jnp.broadcast_to(halos[t - 1, 0, y, pl.ds(x, 1), :], (depth, levels))
            high = jnp.broadcast_to(halos[t - 1, 1, y, pl.ds(x, 1), :], (depth, levels))
            low = jnp.where(on_first, low, pltpu.roll(mid, 1, 0))
            high = jnp.where(on_last, high, pltpu.roll(mid, depth - 1, 0))
            own = at(x, 0)
            spread = (north + south_of) + (west + east_of) + (low + high) - 6.0 * mid
            value = (mid - fy[y, own, :] * (south_of - north) - fx[y, own, :] * (east_of - west)
                     - fz[y, own, :] * (high - low) + 0.05 * spread)
            if t < STEPS:
                u[t, y + 1, at(x, 1), :] = value
            else:
                end[y, own, :] = value
                hop = 1
                while hop < depth:
                    value = value + jnp.where(place_in_block >= hop, pltpu.roll(value, hop, 0), 0.0)
                    hop *= 2
                pot[y, own, :] = value
        if t < STEPS:
            take_faces(t, y, x0)
        else:
            start = x0 * depth + depth - 1
            totals[y, pl.ds(x0, group), :] = pot[y, pl.ds(start, group, stride=depth), :]

    def over(y0, count, x0, span, body):
        groups = span // group

        def one(i, carry):
            body(y0 + i // groups, pl.multiple_of(x0 + (i % groups) * group, group))
            return carry

        lax.fori_loop(0, count * groups, one, 0)

    def finish(y, x0):
        for g in range(group):
            own = pl.ds(pl.multiple_of((x0 + g) * depth, 8), depth)
            value = pot[y, own, :]
            for hop in range(1, sizes["down"]):
                below = jnp.broadcast_to(totals_in[hop - 1, y, pl.ds(x0 + g, 1), :], (depth, levels))
                value = value + jnp.where(places["down"] >= hop, below, 0.0)
            pot[y, own, :] = value * (1.0 / (depth * sizes["down"]))

    down_hops = range(1, sizes["down"])

    def finish_rim(c):
        for side in (0, 1):
            for hop in down_hops:
                rim_total(hop, side, c).wait_recv()
            over(0 if side == 0 else rows - 1, 1, c * width, width, finish)

    def each_chunk(body):
        def one(c, carry):
            body(c)
            return carry

        lax.fori_loop(0, chunks, one, 0)

    def send_chunk(t, c):
        for side in (0, 1):
            south(t, side, c).start()

    each_chunk(lambda c: send_chunk(0, c))
    for part in (0, 1, 2):
        for side in (0, 1):
            east(0, side, part).start()
    loads[0].wait()
    for part in (0, 1, 2):
        over(*blocks[part], 0, columns, functools.partial(take_faces, 0))
        for side in (0, 1):
            down(0, side, part).start()
    for load in loads[1:]:
        load.wait()

    for t in range(1, STEPS + 1):
        for side in (0, 1):
            east(t - 1, side, 0).wait_recv()
            down(t - 1, side, 0).wait_recv()
        over(*blocks[0], 0, columns, functools.partial(march, t))
        if t < STEPS:
            for side in (0, 1):
                east(t, side, 0).start()
                down(t, side, 0).start()
        else:
            for hop in down_hops:
                inner_total(hop).start()
            for hop in down_hops:
                inner_total(hop).wait_recv()
            over(*blocks[0], 0, columns, finish)
        for part in (1, 2):
            for side in (0, 1):
                east(t - 1, side, part).wait_recv()
                down(t - 1, side, part).wait_recv()

        def rim(c):
            for side in (0, 1):
                south(t - 1, side, c).wait_recv()
                y = 0 if side == 0 else rows - 1
                over(y, 1, c * width, width, functools.partial(march, t))
                if t == STEPS:
                    for hop in down_hops:
                        rim_total(hop, side, c).start()
            if t < STEPS:
                send_chunk(t, c)
            else:
                pl.when(c > 0)(lambda: finish_rim(c - 1))

        each_chunk(rim)
        if t < STEPS:
            for part in (1, 2):
                for side in (0, 1):
                    east(t, side, part).start()
                    down(t, side, part).start()
    finish_rim(chunks - 1)
    for t in range(STEPS):
        each_chunk(lambda c: [south(t, side, c).wait_send() for side in (0, 1)])
        for part in (0, 1, 2):
            for side in (0, 1):
                east(t, side, part).wait_send()
                down(t, side, part).wait_send()
    for hop in down_hops:
        inner_total(hop).wait_send()
        each_chunk(lambda c: [rim_total(hop, side, c).wait_send() for side in (0, 1)])


def write_out(*refs):
    count = len(refs) // 2
    sems = refs[-1]
    pairs = zip(refs[:count], refs[count:-1])
    copies = [pltpu.make_async_copy(src, dst, sems.at[i]) for i, (src, dst) in enumerate(pairs)]
    for copy in copies:
        copy.start()
    for copy in copies:
        copy.wait()


def local(sizes, field_values, *flows):
    rows, columns, depth, levels = field_values.shape
    cells = columns * depth
    width = chunk_of(columns, group_of(columns))
    flat = [array.reshape(rows, cells, levels) for array in (field_values, *flows)]
    block = pltpu.VMEM((rows, cells, levels), jnp.float32)
    dma = pltpu.SemaphoreType.DMA
    south_sems, side_sems = (STEPS, 2, columns // width), (STEPS, 2, 3)
    others = sizes["down"] - 1
    face = (rows, columns, levels)
    out = jax.ShapeDtypeStruct((rows, cells, levels), jnp.float32)
    width_sems = (others, 1 + 2 * (columns // width))
    held = pl.pallas_call(
        functools.partial(kernel, sizes, depth),
        out_shape=(block, block),
        in_specs=[pl.BlockSpec(memory_space=pl.ANY)] * 4,
        out_specs=(pl.BlockSpec(memory_space=pltpu.VMEM),) * 2,
        scratch_shapes=[
            pltpu.VMEM((STEPS, rows + 2, cells + 2 * depth, levels), jnp.float32),
            block, block, block,
            pltpu.VMEM((STEPS, 2, *face), jnp.float32),
            pltpu.VMEM((STEPS, 2, *face), jnp.float32),
            pltpu.VMEM(face, jnp.float32),
            pltpu.VMEM((others, *face), jnp.float32),
            dma((4,)),
            dma(south_sems), dma(south_sems),
            dma(side_sems), dma(side_sems),
            dma(side_sems), dma(side_sems),
            dma(width_sems), dma(width_sems),
        ],
        compiler_params=pltpu.CompilerParams(
            collective_id=0, has_side_effects=True, vmem_limit_bytes=48 * 1024 * 1024),
    )(*flat)
    results = pl.pallas_call(
        write_out,
        out_shape=(out, out),
        in_specs=[pl.BlockSpec(memory_space=pltpu.VMEM)] * 2,
        out_specs=(pl.BlockSpec(memory_space=pltpu.HBM),) * 2,
        scratch_shapes=[dma((2,))],
        compiler_params=pltpu.CompilerParams(vmem_limit_bytes=8 * 1024 * 1024),
    )(*held)
    return tuple(array.reshape(rows, columns, depth, levels) for array in results)


def solution(mesh):
    spec = P("south", "east", "down", None)
    sizes = {axis: mesh.shape[axis] for axis in AXES}
    return jax.shard_map(
        functools.partial(local, sizes), mesh=mesh, in_specs=(spec,) * 4,
        out_specs=(spec, spec), check_vma=False)
```

```python
import functools

import jax
import jax.numpy as jnp
from jax import lax
from jax.experimental import pallas as pl
from jax.experimental.pallas import tpu as pltpu
from jax.sharding import PartitionSpec as P

STEPS = 4
AXES = ("south", "east", "down")
MESH = pl.DeviceIdType.MESH


def group_of(columns):
    return next(size for size in (8, 4, 2, 1) if columns % size == 0)


def chunk_of(columns, group):
    return next(size for size in (4 * group, 2 * group, group) if columns % size == 0)


def kernel(sizes, depth, field, flow_y, flow_x, flow_z, pot, end, u, fy, fx, fz,
           faces, halos, totals, totals_in, load_sem, south_send, south_recv,
           east_send, east_recv, down_send, down_recv, tot_send, tot_recv):
    rows, cells, levels = field.shape
    columns = cells // depth
    group = group_of(columns)
    width = chunk_of(columns, group)
    chunks = columns // width
    places = {axis: lax.axis_index(axis) for axis in AXES}

    def beside(axis, hop):
        return {axis: lax.rem(places[axis] + hop, sizes[axis])}

    hops = [(axis, hop) for axis in ("south", "east") for hop in sorted({1, sizes[axis] - 1})]
    hops += [("down", hop) for hop in range(1, sizes["down"])]
    barrier = pltpu.get_barrier_semaphore()
    for axis, hop in hops:
        pl.semaphore_signal(barrier, inc=1, device_id=beside(axis, hop), device_id_type=MESH)

    flows = ((flow_y, fy), (flow_x, fx), (flow_z, fz))
    loads = [
        pltpu.make_async_copy(
            field.at[pl.ds(start, count)], u.at[0, pl.ds(start + 1, count), pl.ds(depth, cells), :],
            load_sem.at[i])
        for i, (start, count) in enumerate(((0, 1), (rows - 1, 1), (1, rows - 2)))]
    loads += [pltpu.make_async_copy(src, dst, load_sem.at[3 + i]) for i, (src, dst) in enumerate(flows)]
    for load in loads[:2]:
        load.start()
    for load in loads[:2]:
        load.wait()
    pl.semaphore_wait(barrier, len(hops))

    def south(t, side, c):
        row = rows - 1 if side == 0 else 0
        at = pl.multiple_of(c * width * depth, 8)
        return pltpu.make_async_remote_copy(
            src_ref=u.at[t, row + 1, pl.ds(at + depth, width * depth), :],
            dst_ref=u.at[t, 0 if side == 0 else rows + 1, pl.ds(at + depth, width * depth), :],
            send_sem=south_send.at[t, side, c], recv_sem=south_recv.at[t, side, c],
            device_id=beside("south", 1 if side == 0 else sizes["south"] - 1), device_id_type=MESH)

    blocks = ((1, rows - 2), (0, 1), (rows - 1, 1))

    def east(t, side, part):
        start, count = blocks[part]
        column = columns if side == 0 else 1
        if t == 0:
            src = field.at[pl.ds(start, count), pl.ds((column - 1) * depth, depth), :]
        else:
            src = u.at[t, pl.ds(start + 1, count), pl.ds(column * depth, depth), :]
        return pltpu.make_async_remote_copy(
            src_ref=src,
            dst_ref=u.at[t, pl.ds(start + 1, count), pl.ds(0 if side == 0 else cells + depth, depth), :],
            send_sem=east_send.at[t, side, part], recv_sem=east_recv.at[t, side, part],
            device_id=beside("east", 1 if side == 0 else sizes["east"] - 1), device_id_type=MESH)

    def down(t, side, part):
        start, count = blocks[part]
        return pltpu.make_async_remote_copy(
            src_ref=faces.at[t, side, pl.ds(start, count)],
            dst_ref=halos.at[t, side, pl.ds(start, count)],
            send_sem=down_send.at[t, side, part], recv_sem=down_recv.at[t, side, part],
            device_id=beside("down", 1 if side == 0 else sizes["down"] - 1), device_id_type=MESH)

    def total(hop, piece, y0, count, x0, span):
        cut = (pl.ds(y0, count), pl.ds(x0, span))
        return pltpu.make_async_remote_copy(
            src_ref=totals.at[cut], dst_ref=totals_in.at[(hop - 1, *cut)],
            send_sem=tot_send.at[hop - 1, piece], recv_sem=tot_recv.at[hop - 1, piece],
            device_id=beside("down", hop), device_id_type=MESH)

    def inner_total(hop):
        return total(hop, 0, *blocks[0], 0, columns)

    def rim_total(hop, side, c):
        at = pl.multiple_of(c * width, group)
        return total(hop, 1 + side * chunks + c, 0 if side == 0 else rows - 1, 1, at, width)

    place_in_block = lax.broadcasted_iota(jnp.int32, (depth, levels), 0)
    on_first, on_last = place_in_block == 0, place_in_block == depth - 1

    def take_faces(t, y, x0):
        for side, place in ((0, depth - 1), (1, 0)):
            start = (x0 + 1) * depth + place
            faces[t, side, y, pl.ds(x0, group), :] = u[t, y + 1, pl.ds(start, group, stride=depth), :]

    def march(t, y, x0):
        def at(x, pad):
            return pl.ds(pl.multiple_of((x + pad) * depth, 8), depth)

        line = [u[t - 1, y + 1, at(x0 + g, 0), :] for g in range(group + 2)]
        for g in range(group):
            x = x0 + g
            mid, west, east_of = line[g + 1], line[g], line[g + 2]
            north, south_of = u[t - 1, y, at(x, 1), :], u[t - 1, y + 2, at(x, 1), :]
            low = jnp.broadcast_to(halos[t - 1, 0, y, pl.ds(x, 1), :], (depth, levels))
            high = jnp.broadcast_to(halos[t - 1, 1, y, pl.ds(x, 1), :], (depth, levels))
            low = jnp.where(on_first, low, pltpu.roll(mid, 1, 0))
            high = jnp.where(on_last, high, pltpu.roll(mid, depth - 1, 0))
            own = at(x, 0)
            spread = (north + south_of) + (west + east_of) + (low + high) - 6.0 * mid
            value = (mid - fy[y, own, :] * (south_of - north) - fx[y, own, :] * (east_of - west)
                     - fz[y, own, :] * (high - low) + 0.05 * spread)
            if t < STEPS:
                u[t, y + 1, at(x, 1), :] = value
            else:
                end[y, own, :] = value
                hop = 1
                while hop < depth:
                    value = value + jnp.where(place_in_block >= hop, pltpu.roll(value, hop, 0), 0.0)
                    hop *= 2
                pot[y, own, :] = value
        if t < STEPS:
            take_faces(t, y, x0)
        else:
            start = x0 * depth + depth - 1
            totals[y, pl.ds(x0, group), :] = pot[y, pl.ds(start, group, stride=depth), :]

    def over(y0, count, x0, span, body):
        groups = span // group

        def one(i, carry):
            body(y0 + i // groups, pl.multiple_of(x0 + (i % groups) * group, group))
            return carry

        lax.fori_loop(0, count * groups, one, 0)

    def finish(y, x0):
        for g in range(group):
            own = pl.ds(pl.multiple_of((x0 + g) * depth, 8), depth)
            value = pot[y, own, :]
            for hop in range(1, sizes["down"]):
                below = jnp.broadcast_to(totals_in[hop - 1, y, pl.ds(x0 + g, 1), :], (depth, levels))
                value = value + jnp.where(places["down"] >= hop, below, 0.0)
            pot[y, own, :] = value * (1.0 / (depth * sizes["down"]))

    down_hops = range(1, sizes["down"])

    def finish_rim(c):
        for side in (0, 1):
            for hop in down_hops:
                rim_total(hop, side, c).wait_recv()
            over(0 if side == 0 else rows - 1, 1, c * width, width, finish)

    def each_chunk(body):
        def one(c, carry):
            body(c)
            return carry

        lax.fori_loop(0, chunks, one, 0)

    def send_chunk(t, c):
        for side in (0, 1):
            south(t, side, c).start()

    each_chunk(lambda c: send_chunk(0, c))
    for load in loads[2:]:
        load.start()
    for part in (0, 1, 2):
        for side in (0, 1):
            east(0, side, part).start()
    loads[2].wait()
    for part in (0, 1, 2):
        over(*blocks[part], 0, columns, functools.partial(take_faces, 0))
        for side in (0, 1):
            down(0, side, part).start()
    for load in loads[3:]:
        load.wait()

    for t in range(1, STEPS + 1):
        for side in (0, 1):
            east(t - 1, side, 0).wait_recv()
            down(t - 1, side, 0).wait_recv()
        over(*blocks[0], 0, columns, functools.partial(march, t))
        if t < STEPS:
            for side in (0, 1):
                east(t, side, 0).start()
                down(t, side, 0).start()
        else:
            for hop in down_hops:
                inner_total(hop).start()
            for hop in down_hops:
                inner_total(hop).wait_recv()
            over(*blocks[0], 0, columns, finish)
        for part in (1, 2):
            for side in (0, 1):
                east(t - 1, side, part).wait_recv()
                down(t - 1, side, part).wait_recv()

        def rim(c):
            for side in (0, 1):
                south(t - 1, side, c).wait_recv()
                y = 0 if side == 0 else rows - 1
                over(y, 1, c * width, width, functools.partial(march, t))
                if t == STEPS:
                    for hop in down_hops:
                        rim_total(hop, side, c).start()
            if t < STEPS:
                send_chunk(t, c)
            else:
                pl.when(c > 0)(lambda: finish_rim(c - 1))

        each_chunk(rim)
        if t < STEPS:
            for part in (1, 2):
                for side in (0, 1):
                    east(t, side, part).start()
                    down(t, side, part).start()
    finish_rim(chunks - 1)
    for t in range(STEPS):
        each_chunk(lambda c: [south(t, side, c).wait_send() for side in (0, 1)])
        for part in (0, 1, 2):
            for side in (0, 1):
                east(t, side, part).wait_send()
                down(t, side, part).wait_send()
    for hop in down_hops:
        inner_total(hop).wait_send()
        each_chunk(lambda c: [rim_total(hop, side, c).wait_send() for side in (0, 1)])


def write_out(*refs):
    count = len(refs) // 2
    sems = refs[-1]
    pairs = zip(refs[:count], refs[count:-1])
    copies = [
        pltpu.make_async_copy(src.at[row], dst.at[row], sems.at[i, row])
        for i, (src, dst) in enumerate(pairs) for row in range(src.shape[0])]
    for copy in copies:
        copy.start()
    for copy in copies:
        copy.wait()


def local(sizes, field_values, *flows):
    rows, columns, depth, levels = field_values.shape
    cells = columns * depth
    width = chunk_of(columns, group_of(columns))
    flat = [array.reshape(rows, cells, levels) for array in (field_values, *flows)]
    block = pltpu.VMEM((rows, cells, levels), jnp.float32)
    dma = pltpu.SemaphoreType.DMA
    south_sems, side_sems = (STEPS, 2, columns // width), (STEPS, 2, 3)
    others = sizes["down"] - 1
    face = (rows, columns, levels)
    out = jax.ShapeDtypeStruct((rows, cells, levels), jnp.float32)
    width_sems = (others, 1 + 2 * (columns // width))
    held = pl.pallas_call(
        functools.partial(kernel, sizes, depth),
        out_shape=(block, block),
        in_specs=[pl.BlockSpec(memory_space=pl.ANY)] * 4,
        out_specs=(pl.BlockSpec(memory_space=pltpu.VMEM),) * 2,
        scratch_shapes=[
            pltpu.VMEM((STEPS, rows + 2, cells + 2 * depth, levels), jnp.float32),
            block, block, block,
            pltpu.VMEM((STEPS, 2, *face), jnp.float32),
            pltpu.VMEM((STEPS, 2, *face), jnp.float32),
            pltpu.VMEM(face, jnp.float32),
            pltpu.VMEM((others, *face), jnp.float32),
            dma((6,)),
            dma(south_sems), dma(south_sems),
            dma(side_sems), dma(side_sems),
            dma(side_sems), dma(side_sems),
            dma(width_sems), dma(width_sems),
        ],
        compiler_params=pltpu.CompilerParams(
            collective_id=0, has_side_effects=True, vmem_limit_bytes=48 * 1024 * 1024),
    )(*flat)
    results = pl.pallas_call(
        write_out,
        out_shape=(out, out),
        in_specs=[pl.BlockSpec(memory_space=pltpu.VMEM)] * 2,
        out_specs=(pl.BlockSpec(memory_space=pltpu.HBM),) * 2,
        scratch_shapes=[dma((2, rows))],
        compiler_params=pltpu.CompilerParams(vmem_limit_bytes=8 * 1024 * 1024),
    )(*held)
    return tuple(array.reshape(rows, columns, depth, levels) for array in results)


def solution(mesh):
    spec = P("south", "east", "down", None)
    sizes = {axis: mesh.shape[axis] for axis in AXES}
    return jax.shard_map(
        functools.partial(local, sizes), mesh=mesh, in_specs=(spec,) * 4,
        out_specs=(spec, spec), check_vma=False)
```
